32 devices in a mesh: dp: 8 (over z, y), mp: 4 (over x, core).
Axes of the slice: x: 2, y: 2, z: 4, core: 2. Of those that a mesh axis runs over, the one named last changes fastest.
Arguments:
- tokens: bfloat16 [6144, 768], P(('dp', 'mp')), may hold values from -6 to 6
- obs_mask: int32 [96, 64], P(('dp', 'mp')), may hold values 0 or 1
- norm_gains: float32 [5, 768], replicated, may hold values from 0.1 to 1.9
- attn_in: bfloat16 [2, 3, 768, 768], P(None, None, 'dp', 'mp'), may hold values from -0.21875 to 0.21875
- attn_out: bfloat16 [2, 768, 768], P(None, 'mp', 'dp'), may hold values from -0.21875 to 0.21875
- mlp_in: bfloat16 [2, 768, 3072], P(None, 'dp', 'mp'), may hold values from -0.21875 to 0.21875
- mlp_out: bfloat16 [2, 3072, 768], P(None, 'mp', 'dp'), may hold values from -0.109375 to 0.109375
- embodiment: int32 [96, 1], P('dp'), may hold values from 0 to 24; in each aligned block of 12 rows (0 to 11, 12 to 23, ...) no two rows name the same one
- levels: int32 [96, 2], P('dp'), may hold values from 0 to 19
- actions: bfloat16 [96, 2, 56], P('dp'), may hold values from -1 to 1
- noise: bfloat16 [96, 2, 56], P('dp'), may hold values from -5 to 5
- action_dims: int32 [25], replicated, may hold values from 7 to 14
- head_read: bfloat16 [32, 768, 256], P('dp'), may hold values from -0.21875 to 0.21875
- head_act: bfloat16 [32, 56, 256], P('dp'), may hold values from -0.75 to 0.75
- time_table: bfloat16 [32, 20, 256], P('dp'), may hold values from -5 to 5
- block_in: bfloat16 [32, 256, 256], P('dp'), may hold values from -0.375 to 0.375
- block_out: bfloat16 [32, 256, 256], P('dp'), may hold values from -0.375 to 0.375
- head_out: bfloat16 [32, 256, 56], P('dp'), may hold values from -0.375 to 0.375
Outputs:
- readout_grad: bfloat16 [96, 2, 768], P(('dp', 'mp'))
- grad_read: float32 [32, 768, 256], P('dp', 'mp')
- grad_act: float32 [32, 56, 256], P('dp')
- grad_time: float32 [32, 20, 256], P('dp')
- grad_block_in: float32 [32, 256, 256], P('dp')
- grad_block_out: float32 [32, 256, 256], P('dp')
- grad_head_out: float32 [32, 256, 56], P('dp')
The draws below stay inside these ranges and needn't reach their ends.
Inputs may be any that keep to these rules, and one draw needn't show every extreme that they name: Within each aligned block of 12 samples (those of one dp index) no embodiment appears twice; every embodiment appears in some block.
All inputs are finite; a program needn't handle non-finite values. No bound on the sum of `obs_mask` on one device may be relied on, other than what follows from the above.
Results may differ from the reference program's by a relative error of at most 0.024.
Values may be sent and summed in bfloat16 or wider, within the bound.
A program may use at most 64 MiB of HBM per device.

```python
import math
import jax
import jax.numpy as jnp
import numpy as np
from jax import lax

D = 768
HEADS = 12
HDIM = 64
FF = 3072
HID = 256
EMB = 25
LAYERS = 2
SEQ = 64
READ = 2
LEVELS = 20
ADIM_MAX = 14
SAMP_DEV = 12
SAMPLES = 96
TOKENS = 6144
EMB_SLOTS = 32
ACT = 56
N_DP = 8
N_MP = 4


def set_ends(result, key, smallest, high):
    dims = result.shape
    place = [jax.random.randint(jax.random.fold_in(key, axis), (), 0, dims[axis]) for axis in range(len(dims))]
    result = result.at[tuple(place)].set(smallest)
    longest = dims.index(max(dims))
    place[longest] = (place[longest] + 1) % dims[longest]
    return result.at[tuple(place)].set(high)


def steps_of(rng, shape, split, least, largest):
    gain, own = 1.0, jax.random.fold_in(rng, 6)
    for axis_at, parts in split:
        draws = jnp.exp(jax.random.uniform(jax.random.fold_in(own, axis_at), (parts,), jnp.float32, least / len(split), largest / len(split)))
        gain = gain * jnp.repeat(draws, shape[axis_at] // parts).reshape([-1 if axis == axis_at else 1 for axis in range(len(shape))])
    return gain


def routed_block(rng, own, number, rows, count, top, reach, lean):
    ranking = jax.random.permutation(rng, count)
    crowded, usual = load_shares(count, rows * top, reach, lean, True), load_shares(count, rows * top, reach, lean, False)
    places = jnp.arange(count)

    def named(lengths, rotation):
        used = int((lengths > 0).sum())
        fixed = max(1, used // 4)
        shifted = fixed + (places - fixed + rotation * (used - fixed)) % max(1, count - fixed)
        return jnp.zeros((count,), jnp.int32).at[ranking[jnp.where(places < fixed, places, shifted)]].set(jnp.asarray(lengths, jnp.int32))

    lengths = jnp.where(number % 4 == 0, named(crowded, number // 4), named(usual, number - number // 4 - 1))
    mixed = jax.random.permutation(jax.random.fold_in(own, 3), count)
    donor, taker = mixed[0:count // 2 * 2:2], mixed[1:count // 2 * 2:2]
    room = jnp.minimum(lengths[donor] - 1, reach - lengths[taker]) // 2
    room = jnp.where((donor == ranking[0]) | (taker == ranking[0]) | (lengths[taker] == 0), 0, jnp.maximum(room, 0))
    shifted = jax.random.randint(jax.random.fold_in(own, 4), (count // 2,), 0, 1 << 20) % (room + 1)
    lengths = lengths.at[donor].add(-shifted).at[taker].add(shifted)
    items = jnp.searchsorted(jnp.cumsum(lengths), jnp.arange(rows * top), side="right").astype(jnp.int32)
    grid = items.reshape(top, rows).T
    grid = grid[jax.random.permutation(jax.random.fold_in(own, 1), rows)]
    rotation = jax.random.randint(jax.random.fold_in(own, 2), (rows, 1), 0, top)
    return jnp.take_along_axis(grid, (jnp.arange(top)[None, :] + rotation) % top, axis=1)


def load_shares(count, total, reach, lean, full):
    weights = [(1 << 20) // math.isqrt(grade ** lean) + 1 for grade in range(1, count + 1)]
    largest = reach if full else min(reach, max(-(-total // count), total * weights[0] // sum(weights)))
    least = 1 if total - largest >= count - 1 else 0
    counts, surplus = [largest] + [least] * (count - 1), total - largest - least * (count - 1)
    while surplus > 0:
        movable = [i for i in range(1, count) if counts[i] < largest] or [i for i in range(1, count) if counts[i] < reach]
        whole, remaining = sum([weights[i] for i in movable]), surplus
        for i in movable:
            addition = min(reach - counts[i], max(1, remaining * weights[i] // whole), surplus)
            counts[i] = counts[i] + addition
            surplus = surplus - addition
    return np.array(counts)


def bell_draw(rng, dims, scale, reach, shards=(), kind=jnp.bfloat16):
    values = scale * jax.random.normal(rng, dims, jnp.float32)
    if shards:
        values = values * steps_of(rng, dims, shards, -0.22, 0.18)
    return jnp.clip(values, -reach, reach).astype(kind)


def setup_inputs(seed: int = 0) -> dict:
    arg_keys = jax.random.split(jax.random.key(seed), 19)
    tokens = bell_draw(arg_keys[0], (TOKENS, D), 1.0, 6.0, ((0, 32),))
    obs_mask = set_ends((jax.random.randint(arg_keys[1], (SAMPLES, SEQ), 0, 4) < 3).astype(jnp.int32), jax.random.fold_in(arg_keys[1], 1), 0, 1)
    norm_gains = jnp.clip(1.0 + 0.18 * jax.random.normal(arg_keys[2], (2 * LAYERS + 1, D), jnp.float32), 0.1, 1.9)
    attn_in = bell_draw(arg_keys[3], (LAYERS, 3, D, D), D ** -0.5, 0.21875, ((2, 8), (3, 4)))
    attn_out = bell_draw(arg_keys[4], (LAYERS, D, D), D ** -0.5, 0.21875, ((1, 4), (2, 8)))
    mlp_in = bell_draw(arg_keys[5], (LAYERS, D, FF), D ** -0.5, 0.21875, ((1, 8), (2, 4)))
    mlp_out = bell_draw(arg_keys[6], (LAYERS, FF, D), FF ** -0.5, 0.109375, ((1, 4), (2, 8)))
    embodiment_keys = jax.random.split(jax.random.fold_in(arg_keys[7], 1), SAMPLES // SAMP_DEV)
    embodiment_turns = jax.random.permutation(jax.random.fold_in(arg_keys[7], 3), SAMPLES // SAMP_DEV)
    embodiment = jax.vmap(lambda own, number: routed_block(jax.random.fold_in(arg_keys[7], 2), own, number, SAMP_DEV, EMB, 1, 1, 2))(embodiment_keys, embodiment_turns).reshape((SAMPLES, 1))
    levels = set_ends(jax.random.randint(arg_keys[8], (SAMPLES, READ), 0, LEVELS), jax.random.fold_in(arg_keys[8], 1), 0, LEVELS - 1).astype(jnp.int32)
    actions = jnp.clip(jax.random.uniform(arg_keys[9], (SAMPLES, READ, ACT), jnp.float32, -1.0, 1.0) * steps_of(arg_keys[9], (SAMPLES, READ, ACT), ((0, 8),), -0.4, 0.0), -1.0, 1.0).astype(jnp.bfloat16)
    noise = bell_draw(arg_keys[10], (SAMPLES, READ, ACT), 1.0, 5.0, ((0, 8),))
    action_dims = set_ends(jax.random.randint(arg_keys[11], (EMB,), 7, ADIM_MAX + 1), jax.random.fold_in(arg_keys[11], 1), 7, ADIM_MAX).astype(jnp.int32)
    head_read = bell_draw(arg_keys[12], (EMB_SLOTS, D, HID), D ** -0.5, 0.21875, ((0, 8),))
    head_act = bell_draw(arg_keys[13], (EMB_SLOTS, ACT, HID), ACT ** -0.5, 0.75, ((0, 8),))
    time_table = bell_draw(arg_keys[14], (EMB_SLOTS, LEVELS, HID), 1.0, 5.0, ((0, 8),))
    block_in = bell_draw(arg_keys[15], (EMB_SLOTS, HID, HID), HID ** -0.5, 0.375, ((0, 8),))
    block_out = bell_draw(arg_keys[16], (EMB_SLOTS, HID, HID), HID ** -0.5, 0.375, ((0, 8),))
    head_out = bell_draw(arg_keys[17], (EMB_SLOTS, HID, ACT), HID ** -0.5, 0.375, ((0, 8),))
    return {"tokens": tokens, "obs_mask": obs_mask, "norm_gains": norm_gains, "attn_in": attn_in, "attn_out": attn_out, "mlp_in": mlp_in, "mlp_out": mlp_out, "embodiment": embodiment, "levels": levels, "actions": actions, "noise": noise, "action_dims": action_dims, "head_read": head_read, "head_act": head_act, "time_table": time_table, "block_in": block_in, "block_out": block_out, "head_out": head_out}


norm_eps = 1e-05

def normalize(values, scale_gain):
    center = values - lax.optimization_barrier(jnp.mean(values, axis=-1, keepdims=True))
    spread = lax.optimization_barrier(jnp.mean(center * center, axis=-1, keepdims=True))
    return center * lax.rsqrt(spread + norm_eps) * scale_gain

def allowed_keys(observed):
    length = observed.shape[1]
    position = jnp.arange(length)
    visible = (observed == 1) & (position < length - READ)[None, :]
    itself = position[:, None] == position[None, :]
    return visible[:, None, :] | itself[None, :, :]

def attend(queries, key_rows, value_rows, allowed):
    scores = jnp.einsum('sqhd,skhd->shqk', queries.astype(jnp.float32), key_rows.astype(jnp.float32)) * HDIM ** (-0.5)
    weights = jnp.where(allowed[:, None, :, :], jnp.exp(scores), 0.0)
    shares = (weights / lax.optimization_barrier(jnp.sum(weights, axis=-1, keepdims=True))).astype(jnp.bfloat16)
    context = jnp.einsum('shqk,skhd->sqhd', shares.astype(jnp.float32), value_rows.astype(jnp.float32))
    return context.astype(jnp.bfloat16)

def split_sum(left_side, right_side, groups):
    part_width = left_side.shape[1] // groups
    summed = jnp.zeros((left_side.shape[0], right_side.shape[1]), jnp.float32)
    for part_index in range(groups):
        lower = part_index * part_width
        partial_value = jnp.dot(left_side[:, lower:lower + part_width], right_side[lower:lower + part_width], preferred_element_type=jnp.float32)
        summed = summed + lax.optimization_barrier(partial_value.astype(jnp.bfloat16)).astype(jnp.float32)
    return summed

def trunk_block(inputs, observed, norm_gains, attn_in, attn_out, mlp_in, mlp_out):
    residual = inputs.astype(jnp.float32)
    allowed = allowed_keys(observed)
    samples = observed.shape[0]
    for layer_index in range(LAYERS):
        normed = normalize(residual, norm_gains[2 * layer_index]).astype(jnp.bfloat16)
        projected = [jnp.dot(normed, attn_in[layer_index, member], preferred_element_type=jnp.float32).astype(jnp.bfloat16).reshape(samples, SEQ, HEADS, HDIM) for member in range(3)]
        context = attend(projected[0], projected[1], projected[2], allowed).reshape(-1, D)
        residual = residual + split_sum(context, attn_out[layer_index], N_MP)
        normed = normalize(residual, norm_gains[2 * layer_index + 1]).astype(jnp.bfloat16)
        hidden = jax.nn.gelu(jnp.dot(normed, mlp_in[layer_index], preferred_element_type=jnp.float32), approximate=True).astype(jnp.bfloat16)
        residual = residual + split_sum(hidden, mlp_out[layer_index], N_MP)
    ending = residual.reshape(samples, SEQ, D)[:, SEQ - READ:, :]
    return normalize(ending, norm_gains[2 * LAYERS]).astype(jnp.bfloat16)

def plan():
    steps_up = (jnp.arange(LEVELS, dtype=jnp.float32) + 1.0) / LEVELS
    anchor = math.cos(0.008 / 1.008 * math.pi / 2) ** 2
    return jnp.cos((steps_up + 0.008) / 1.008 * (math.pi / 2)) ** 2 / anchor

def noisy_pair(level_ids, clean, noise_draw, table):
    picked = (level_ids[..., None] == jnp.arange(LEVELS)).astype(jnp.float32)
    kept = lax.optimization_barrier(jnp.sum(picked * table, axis=-1))[..., None]
    mixed = jnp.sqrt(kept) * clean.astype(jnp.float32) + jnp.sqrt(1.0 - kept) * noise_draw.astype(jnp.float32)
    return mixed.astype(jnp.bfloat16)

def tail(first, target, weight_mask, inner_weight, outer_weight, final_weight):
    highest = lax.Precision.HIGHEST
    active = jax.nn.silu(first).astype(jnp.bfloat16)
    inner = jnp.dot(active, inner_weight, preferred_element_type=jnp.float32, precision=highest)
    second = jax.nn.silu(inner).astype(jnp.bfloat16)
    hidden = first + jnp.dot(second, outer_weight, preferred_element_type=jnp.float32, precision=highest)
    third = jax.nn.silu(hidden).astype(jnp.bfloat16)
    predicted = jnp.dot(third, final_weight, preferred_element_type=jnp.float32, precision=highest)
    differ = predicted - target
    return 0.5 * jnp.sum(weight_mask * differ * differ)

def reference(tokens, obs_mask, norm_gains, attn_in, attn_out, mlp_in, mlp_out, embodiment, levels, actions, noise, action_dims, head_read, head_act, time_table, block_in, block_out, head_out):

    def one_block(pieces):
        return trunk_block(pieces[0], pieces[1], norm_gains, attn_in, attn_out, mlp_in, mlp_out)
    blocks = lax.map(one_block, (tokens.reshape(N_DP, SAMP_DEV * SEQ, D), obs_mask.reshape(N_DP, SAMP_DEV, SEQ)))
    readouts = blocks.reshape(-1, D)
    table = plan()
    noisy = noisy_pair(levels, actions, noise, table).reshape(-1, ACT)
    target = noise.reshape(-1, ACT).astype(jnp.float32)
    level_rows = levels.reshape(-1)
    owner_rows = jnp.repeat(embodiment[:, 0], READ)
    one_hot = (level_rows[:, None] == jnp.arange(LEVELS)).astype(jnp.bfloat16)
    column = jnp.arange(ACT) % ADIM_MAX
    slot_count = head_read.shape[0]

    def per_head(carried, slot):
        read_weight = head_read[slot]
        live = (owner_rows == slot).astype(jnp.float32)
        dims_here = jnp.sum(jnp.where(jnp.arange(EMB) == slot, action_dims, 0))
        weight_mask = live[:, None] * (column[None, :] < dims_here).astype(jnp.float32)
        first = jnp.dot(readouts, read_weight, preferred_element_type=jnp.float32)
        first = first + jnp.dot(noisy, head_act[slot], preferred_element_type=jnp.float32)
        first = first + jnp.dot(one_hot, time_table[slot], preferred_element_type=jnp.float32)

        def head_loss(first_in, inner_weight, outer_weight, final_weight):
            return tail(first_in, target, weight_mask, inner_weight, outer_weight, final_weight)
        loss_value, pullback = jax.vjp(head_loss, first, block_in[slot].astype(jnp.float32), block_out[slot].astype(jnp.float32), head_out[slot].astype(jnp.float32))
        grad_first, grad_inner, grad_outer, grad_final = pullback(jnp.ones((), jnp.float32))
        grad_bf = grad_first.astype(jnp.bfloat16)
        grad_readin = jnp.dot(readouts.T, grad_bf, preferred_element_type=jnp.float32)
        grad_actin = jnp.dot(noisy.T, grad_bf, preferred_element_type=jnp.float32)
        grad_timein = jnp.dot(one_hot.T, grad_bf, preferred_element_type=jnp.float32)
        carried = carried + jnp.dot(grad_bf, read_weight.T, preferred_element_type=jnp.float32)
        return (carried, (grad_readin, grad_actin, grad_timein, grad_inner, grad_outer, grad_final))
    returned, grads = lax.scan(per_head, jnp.zeros(readouts.shape, jnp.float32), jnp.arange(slot_count))
    grad_readin, grad_actin, grad_timein, grad_inner, grad_outer, grad_final = grads
    return (returned.astype(jnp.bfloat16).reshape(SAMPLES, READ, D), grad_readin, grad_actin, grad_timein, grad_inner, grad_outer, grad_final)
```

```python
import functools
import math

import jax
import jax.numpy as jnp
from jax import lax
from jax.experimental import pallas as pl
from jax.experimental.pallas import tpu as pltpu
from jax.sharding import PartitionSpec as P

HDIM = 64
EMB = 25
READ = 2
LEVELS = 20
ADIM_MAX = 14

norm_eps = 1e-05
MESH_ID = pl.DeviceIdType.MESH


def normalize(values, scale_gain):
    center = values - jnp.mean(values, axis=-1, keepdims=True)
    spread = jnp.mean(center * center, axis=-1, keepdims=True)
    return center * lax.rsqrt(spread + norm_eps) * scale_gain


def plan():
    steps_up = (jnp.arange(LEVELS, dtype=jnp.float32) + 1.0) / LEVELS
    anchor = math.cos(0.008 / 1.008 * math.pi / 2) ** 2
    return jnp.cos((steps_up + 0.008) / 1.008 * (math.pi / 2)) ** 2 / anchor


def noisy_pair(level_ids, clean, noise_draw, table):
    picked = (level_ids[..., None] == jnp.arange(LEVELS)).astype(jnp.float32)
    kept = jnp.sum(picked * table, axis=-1)[..., None]
    mixed = jnp.sqrt(kept) * clean.astype(jnp.float32) + jnp.sqrt(1.0 - kept) * noise_draw.astype(
        jnp.float32
    )
    return mixed.astype(jnp.bfloat16)


def ring_place(index, size):
    if size % 2:
        return index
    odd = index % 2
    return (1 - odd) * (index // 2) + odd * (size - 1 - index // 2)


def ring_index(place, size):
    if size % 2:
        return place
    back = place // (size // 2)
    return (1 - back) * (2 * place) + back * (2 * (size - 1 - place) + 1)


def ring_parts(rows, tile=16):
    if rows % (2 * tile):
        return [(0, rows)], []
    half = rows // 2
    return [[(way * half + start, tile) for start in range(0, half, tile)] for way in range(2)]


def exchange_kernel(n_dp, n_mp, kinds, *refs):
    count = len(kinds)
    ins, outs = refs[:count], refs[count : 2 * count]
    sems = refs[2 * count :]
    local_sem = sems[-1]
    my_dp, my_mp = lax.axis_index("dp"), lax.axis_index("mp")
    place = ring_place(my_dp, n_dp)

    talk_mp = any(kind in ("split", "cast") for kind in kinds)
    talk_dp = "swap" in kinds
    talk_ring = "ring" in kinds
    barrier = pltpu.get_barrier_semaphore()
    greeted = 0
    if talk_mp:
        for offset in range(1, n_mp):
            pl.semaphore_signal(
                barrier, inc=1, device_id={"mp": (my_mp + offset) % n_mp}, device_id_type=MESH_ID
            )
            greeted += 1
    if talk_dp:
        for offset in range(1, n_dp):
            pl.semaphore_signal(
                barrier, inc=1, device_id={"dp": (my_dp + offset) % n_dp}, device_id_type=MESH_ID
            )
            greeted += 1
    elif talk_ring:
        for way in (1, n_dp - 1):
            pl.semaphore_signal(
                barrier,
                inc=1,
                device_id={"dp": ring_index((place + way) % n_dp, n_dp)},
                device_id_type=MESH_ID,
            )
            greeted += 1
    pl.semaphore_wait(barrier, greeted)

    def ring_copies(item, step):
        source, landing = ins[item], outs[item]
        made = []
        for way, parts in enumerate(ring_parts(source.shape[0])):
            for chunk, (start, extent) in enumerate(parts):
                origin = ring_index((place + (n_dp - step if way == 0 else step)) % n_dp, n_dp)
                target = ring_index((place + (1 if way == 0 else n_dp - 1)) % n_dp, n_dp)
                rows = pl.ds(start, extent)
                spot = landing.at[origin, rows]
                made.append(
                    pltpu.make_async_remote_copy(
                        src_ref=source.at[rows] if step == 0 else spot,
                        dst_ref=spot,
                        send_sem=sems[2 * item].at[step, chunk, way],
                        recv_sem=sems[2 * item + 1].at[step, chunk, way],
                        device_id={"dp": target},
                        device_id_type=MESH_ID,
                    )
                )
        return made

    rings = [item for item in range(count) if kinds[item] == "ring"]
    flights = {item: ring_copies(item, 0) for item in rings}
    for item in rings:
        for copy in flights[item]:
            copy.start()
    direct = []
    keeps = []
    for item, kind in enumerate(kinds):
        source, landing = ins[item], outs[item]
        if kind == "ring":
            keeps.append(pltpu.make_async_copy(source, landing.at[my_dp], local_sem.at[item]))
            continue
        size, mine, axis = (n_dp, my_dp, "dp") if kind == "swap" else (n_mp, my_mp, "mp")
        for offset in range(1, size):
            peer = (mine + offset) % size
            copy = pltpu.make_async_remote_copy(
                src_ref=source if kind == "cast" else source.at[peer],
                dst_ref=landing.at[mine],
                send_sem=sems[2 * item].at[offset],
                recv_sem=sems[2 * item + 1].at[offset],
                device_id={axis: peer},
                device_id_type=MESH_ID,
            )
            copy.start()
            direct.append(copy)
        keeps.append(
            pltpu.make_async_copy(
                source if kind == "cast" else source.at[mine], landing.at[mine], local_sem.at[item]
            )
        )
    for keep in keeps:
        keep.start()
    sent = [copy for item in rings for copy in flights[item]]
    for step in range(1, n_dp - 1):
        for item in rings:
            following = ring_copies(item, step)
            for before, after in zip(flights[item], following):
                before.wait_recv()
                after.start()
            flights[item] = following
            sent = sent + following
    for item in rings:
        for copy in flights[item]:
            copy.wait_recv()
    for copy in direct:
        copy.wait_recv()
    for copy in sent + direct:
        copy.wait_send()
    for keep in keeps:
        keep.wait()


def exchange(ident, *pairs):
    n_dp, n_mp = lax.axis_size("dp"), lax.axis_size("mp")
    kinds = tuple(kind for kind, _ in pairs)
    arrays = [array for _, array in pairs]
    shapes, scratch = [], []
    for kind, array in pairs:
        lead = {"ring": (n_dp,), "cast": (n_mp,), "split": (), "swap": ()}[kind]
        shapes.append(jax.ShapeDtypeStruct(lead + array.shape, array.dtype))
        if kind == "ring":
            slots = (n_dp - 1, len(ring_parts(array.shape[0])[0]), 2)
        else:
            slots = (n_dp if kind == "swap" else n_mp,)
        scratch += [pltpu.SemaphoreType.DMA(slots), pltpu.SemaphoreType.DMA(slots)]
    scratch.append(pltpu.SemaphoreType.DMA((len(pairs),)))
    return pl.pallas_call(
        functools.partial(exchange_kernel, n_dp, n_mp, kinds),
        out_shape=shapes,
        in_specs=[pl.BlockSpec(memory_space=pltpu.VMEM)] * len(pairs),
        out_specs=[pl.BlockSpec(memory_space=pltpu.VMEM)] * len(pairs),
        scratch_shapes=scratch,
        compiler_params=pltpu.CompilerParams(collective_id=ident, has_side_effects=True),
        name="exchange%d" % ident,
    )(*arrays)


def attend(queries, key_rows, value_rows, allowed):
    scores = jnp.einsum(
        "sqhd,skhd->shqk", queries, key_rows, preferred_element_type=jnp.float32
    ) * HDIM ** (-0.5)
    weights = jnp.where(allowed[:, None, :, :], jnp.exp(scores), 0.0)
    shares = (weights / jnp.sum(weights, axis=-1, keepdims=True)).astype(jnp.bfloat16)
    context = jnp.einsum("shqk,skhd->sqhd", shares, value_rows, preferred_element_type=jnp.float32)
    return context.astype(jnp.bfloat16)


def dot32(left, right):
    return jnp.dot(left, right, preferred_element_type=jnp.float32)


def dot_turned(left, right):
    return lax.dot_general(
        left, right, (((1,), (1,)), ((), ())), preferred_element_type=jnp.float32
    )


def added(blocks):
    return jnp.sum(blocks.astype(jnp.float32), axis=0)


def tail(first, target, weight_mask, inner_weight, outer_weight, final_weight):
    highest = lax.Precision.HIGHEST
    active = jax.nn.silu(first).astype(jnp.bfloat16)
    inner = jnp.dot(active, inner_weight, preferred_element_type=jnp.float32, precision=highest)
    second = jax.nn.silu(inner).astype(jnp.bfloat16)
    hidden = first + jnp.dot(
        second, outer_weight, preferred_element_type=jnp.float32, precision=highest
    )
    third = jax.nn.silu(hidden).astype(jnp.bfloat16)
    predicted = jnp.dot(third, final_weight, preferred_element_type=jnp.float32, precision=highest)
    differ = predicted - target
    return 0.5 * jnp.sum(weight_mask * differ * differ)


def head_grads(first, inner_weight, outer_weight, final_weight, target, weight_mask):

    def head_loss(first_in, inner_in, outer_in, final_in):
        return tail(first_in, target, weight_mask, inner_in, outer_in, final_in)

    loss_value, pullback = jax.vjp(head_loss, first, inner_weight, outer_weight, final_weight)
    return pullback(jnp.ones((), jnp.float32))


def on_device(
    tokens,
    obs_mask,
    norm_gains,
    attn_in,
    attn_out,
    mlp_in,
    mlp_out,
    embodiment,
    levels,
    actions,
    noise,
    action_dims,
    head_read,
    head_act,
    time_table,
    block_in,
    block_out,
    head_out,
):
    model = tokens.shape[1]
    act = actions.shape[2]
    width = attn_in.shape[3]
    heads_local = width // HDIM
    samples_local, length = obs_mask.shape
    layer_count = attn_in.shape[0]
    n_mp, n_dp = lax.axis_size("mp"), lax.axis_size("dp")
    my_model, my_owner = lax.axis_index("mp"), lax.axis_index("dp")
    samples_group = samples_local * n_mp
    ident = iter(range(100))

    joined = [
        jnp.concatenate(
            [attn_in[layer, 0], attn_in[layer, 1], attn_in[layer, 2], attn_out[layer].T], axis=1
        )
        for layer in range(layer_count)
    ]
    lowered = [mlp_out[layer].T for layer in range(layer_count)]

    heads_dev = head_read.shape[0]
    slot_count = heads_dev * n_dp
    owners = embodiment[:, 0]
    table = plan()
    onto = (jnp.arange(slot_count)[:, None] == owners[None, :]).astype(jnp.bfloat16)
    spread_rows = jnp.einsum("es,rq->ersq", onto, jnp.eye(READ, dtype=jnp.bfloat16)).reshape(
        slot_count * READ, samples_group * READ
    )
    small = jnp.concatenate(
        [
            noisy_pair(levels, actions, noise, table),
            noise,
            (levels + 1)[..., None].astype(jnp.bfloat16),
        ],
        axis=-1,
    ).reshape(samples_group * READ, 2 * act + 1)
    small = jnp.pad(small, ((0, 0), (0, -small.shape[1] % 128)))
    small = dot32(spread_rows, small).astype(jnp.bfloat16)
    small = small.reshape(n_dp, heads_dev * READ, small.shape[1])

    residual = tokens.astype(jnp.float32)
    wide = None
    allowed = None
    mask_group = None
    got_small = None
    position = jnp.arange(length)
    for layer in range(layer_count):
        final = layer == layer_count - 1
        normed = normalize(residual, norm_gains[2 * layer]).astype(jnp.bfloat16)
        if layer == 0:
            sends = [("cast", normed), ("cast", obs_mask), ("swap", small), ("ring", joined[0])]
        else:
            sends = [("cast", normed)]
        if final:
            ends = residual.reshape(samples_local, length, model)[:, length - READ :, :]
            sends += [("cast", ends), ("ring", mlp_in[layer]), ("ring", lowered[layer])]
        got = list(exchange(next(ident), *sends))
        gathered = got.pop(0).reshape(-1, model)
        if layer == 0:
            mask_group = got.pop(0).reshape(samples_group, length)
            got_small = got.pop(0)
            wide = got.pop(0).reshape(model, -1)
            visible = (mask_group == 1) & (position < length - READ)[None, :]
            itself = position[:, None] == position[None, :]
            allowed = visible[:, None, :] | itself[None, :, :]
        if final:
            ends = got.pop(0).reshape(samples_group * READ, model)
            upper = got.pop(0).reshape(model, -1)
            lower = got.pop(0).reshape(model, -1)
            asking = gathered.reshape(samples_group, length, model)[:, length - READ :, :]
            queries = dot32(asking.reshape(-1, model), wide[:, :width]).astype(jnp.bfloat16)
            queries = queries.reshape(samples_group, READ, heads_local, HDIM)
            both = dot32(gathered, wide[:, width : 3 * width]).astype(jnp.bfloat16)
            keys_at = both[:, :width].reshape(samples_group, length, heads_local, HDIM)
            values_at = both[:, width:].reshape(samples_group, length, heads_local, HDIM)
            context = attend(queries, keys_at, values_at, allowed[:, length - READ :, :])
            partial_value = dot_turned(context.reshape(-1, width), wide[:, 3 * width :])
            (terms,) = exchange(next(ident), ("cast", partial_value.astype(jnp.bfloat16)))
            ends = ends + added(terms)
            normed = normalize(ends, norm_gains[2 * layer + 1]).astype(jnp.bfloat16)
            hidden = jax.nn.gelu(dot32(normed, upper), approximate=True).astype(jnp.bfloat16)
            partial_value = dot_turned(hidden, lower)
            (terms,) = exchange(next(ident), ("cast", partial_value.astype(jnp.bfloat16)))
            ends = ends + added(terms)
            break
        projected = dot32(gathered, wide[:, : 3 * width]).astype(jnp.bfloat16)
        split = [
            projected[:, part * width : (part + 1) * width].reshape(
                samples_group, length, heads_local, HDIM
            )
            for part in range(3)
        ]
        context = attend(split[0], split[1], split[2], allowed).reshape(-1, width)
        partial_value = dot_turned(context, wide[:, 3 * width :]).astype(jnp.bfloat16)
        terms, upper = exchange(
            next(ident),
            ("split", partial_value.reshape(n_mp, -1, model)),
            ("ring", mlp_in[layer]),
        )
        residual = residual + added(terms)
        normed = normalize(residual, norm_gains[2 * layer + 1]).astype(jnp.bfloat16)
        gathered, lower = exchange(next(ident), ("cast", normed), ("ring", lowered[layer]))
        raised = dot32(gathered.reshape(-1, model), upper.reshape(model, -1))
        hidden = jax.nn.gelu(raised, approximate=True).astype(jnp.bfloat16)
        partial_value = dot_turned(hidden, lower.reshape(model, -1)).astype(jnp.bfloat16)
        terms, wide = exchange(
            next(ident),
            ("split", partial_value.reshape(n_mp, -1, model)),
            ("ring", joined[layer + 1]),
        )
        wide = wide.reshape(model, -1)
        residual = residual + added(terms)

    readouts = normalize(ends, norm_gains[2 * layer_count]).astype(jnp.bfloat16)
    send = dot32(spread_rows, readouts).astype(jnp.bfloat16)
    (got_features,) = exchange(
        next(ident), ("swap", send.reshape(n_dp, heads_dev * READ, model))
    )

    def by_head(values):
        values = values.reshape(n_dp, heads_dev, READ, values.shape[-1])
        return jnp.moveaxis(values, 1, 0).reshape(heads_dev, n_dp * READ, values.shape[-1])

    head_features = by_head(got_features)
    head_small = by_head(got_small)
    head_noisy = head_small[..., :act]
    head_target = head_small[..., act : 2 * act].astype(jnp.float32)
    head_levels = head_small[..., 2 * act].astype(jnp.int32) - 1
    head_onehot = (head_levels[..., None] == jnp.arange(LEVELS)).astype(jnp.bfloat16)
    slot_ids = my_owner * heads_dev + jnp.arange(heads_dev)
    dims_here = jnp.sum(
        jnp.where(jnp.arange(EMB)[None, :] == slot_ids[:, None], action_dims[None, :], 0), axis=1
    )
    column = jnp.arange(act) % ADIM_MAX
    weight_mask = (head_levels >= 0).astype(jnp.float32)[..., None] * (
        column[None, None, :] < dims_here[:, None, None]
    ).astype(jnp.float32)
    others = jnp.einsum("hna,hac->hnc", head_noisy, head_act, preferred_element_type=jnp.float32)
    others = others + jnp.einsum(
        "hnl,hlc->hnc", head_onehot, time_table, preferred_element_type=jnp.float32
    )
    first = (
        jnp.einsum("hnd,hdc->hnc", head_features, head_read, preferred_element_type=jnp.float32)
        + others
    )
    grad_first, grad_inner, grad_outer, grad_final = jax.vmap(head_grads)(
        first,
        block_in.astype(jnp.float32),
        block_out.astype(jnp.float32),
        head_out.astype(jnp.float32),
        head_target,
        weight_mask,
    )
    grad_bf = grad_first.astype(jnp.bfloat16)
    backward = jnp.einsum(
        "hnc,hdc->hnd", grad_bf, head_read, preferred_element_type=jnp.float32
    ).astype(jnp.bfloat16)
    backward = jnp.moveaxis(backward.reshape(heads_dev, n_dp, READ, model), 0, 1)
    (arrived,) = exchange(
        next(ident), ("swap", backward.reshape(n_dp, heads_dev * READ, model))
    )
    mine = lax.dynamic_slice_in_dim(
        spread_rows, my_model * (samples_local * READ), samples_local * READ, 1
    )
    returned = lax.dot_general(
        mine,
        arrived.reshape(slot_count * READ, model),
        (((0,), (0,)), ((), ())),
        preferred_element_type=jnp.float32,
    ).astype(jnp.bfloat16)
    feature_width = model // n_mp
    own_features = lax.dynamic_slice_in_dim(
        head_features, my_model * feature_width, feature_width, 2
    )
    grad_readin = jnp.einsum(
        "hnd,hnc->hdc", own_features, grad_bf, preferred_element_type=jnp.float32
    )
    grad_actin = jnp.einsum("hna,hnc->hac", head_noisy, grad_bf, preferred_element_type=jnp.float32)
    grad_timein = jnp.einsum(
        "hnl,hnc->hlc", head_onehot, grad_bf, preferred_element_type=jnp.float32
    )
    return (
        returned.reshape(samples_local, READ, model),
        grad_readin,
        grad_actin,
        grad_timein,
        grad_inner,
        grad_outer,
        grad_final,
    )


def solution(mesh):
    placed = (
        P(("dp", "mp"), None),
        P(("dp", "mp"), None),
        P(),
        P(None, None, "dp", "mp"),
        P(None, "mp", "dp"),
        P(None, "dp", "mp"),
        P(None, "mp", "dp"),
        P("dp", None),
        P("dp", None),
        P("dp", None, None),
        P("dp", None, None),
        P(),
        P("dp", None, None),
        P("dp", None, None),
        P("dp", None, None),
        P("dp", None, None),
        P("dp", None, None),
        P("dp", None, None),
    )
    return jax.shard_map(
        on_device,
        mesh=mesh,
        in_specs=placed,
        out_specs=(
            P(("dp", "mp"), None, None),
            P("dp", "mp", None),
            P("dp", None, None),
            P("dp", None, None),
            P("dp", None, None),
            P("dp", None, None),
            P("dp", None, None),
        ),
        check_vma=False,
    )
```

```python
import functools
import math

import jax
import jax.numpy as jnp
from jax import lax
from jax.experimental import pallas as pl
from jax.experimental.pallas import tpu as pltpu
from jax.sharding import PartitionSpec as P

HDIM = 64
EMB = 25
READ = 2
LEVELS = 20
ADIM_MAX = 14

norm_eps = 1e-05
MESH_ID = pl.DeviceIdType.MESH


def normalize(values, scale_gain):
    center = values - jnp.mean(values, axis=-1, keepdims=True)
    spread = jnp.mean(center * center, axis=-1, keepdims=True)
    return center * lax.rsqrt(spread + norm_eps) * scale_gain


def plan():
    steps_up = (jnp.arange(LEVELS, dtype=jnp.float32) + 1.0) / LEVELS
    anchor = math.cos(0.008 / 1.008 * math.pi / 2) ** 2
    return jnp.cos((steps_up + 0.008) / 1.008 * (math.pi / 2)) ** 2 / anchor


def noisy_pair(level_ids, clean, noise_draw, table):
    picked = (level_ids[..., None] == jnp.arange(LEVELS)).astype(jnp.float32)
    kept = jnp.sum(picked * table, axis=-1)[..., None]
    mixed = jnp.sqrt(kept) * clean.astype(jnp.float32) + jnp.sqrt(1.0 - kept) * noise_draw.astype(
        jnp.float32
    )
    return mixed.astype(jnp.bfloat16)


def ring_place(index, size):
    if size % 2:
        return index
    odd = index % 2
    return (1 - odd) * (index // 2) + odd * (size - 1 - index // 2)


def ring_index(place, size):
    if size % 2:
        return place
    back = place // (size // 2)
    return (1 - back) * (2 * place) + back * (2 * (size - 1 - place) + 1)


def ring_parts(rows, tile=16):
    if rows % tile:
        return [(0, rows)]
    return [(start, tile) for start in range(0, rows, tile)]


def ring_step(parts, step, size):
    count = len(parts)
    if size % 2 == 0 and step == size // 2 - 1:
        near = (count + 1) // 2
        pairs = [(0, chunk) for chunk in range(near)], [(1, chunk) for chunk in range(near, count)]
        mixed = []
        for chunk in range(near):
            mixed += [side[chunk] for side in pairs if chunk < len(side)]
        return mixed
    return [(way, chunk) for chunk in range(count) for way in range(2)]


def exchange_kernel(n_dp, n_mp, kinds, *refs):
    count = len(kinds)
    ins, outs = refs[:count], refs[count : 2 * count]
    sems = refs[2 * count :]
    local_sem = sems[-1]
    my_dp, my_mp = lax.axis_index("dp"), lax.axis_index("mp")
    place = ring_place(my_dp, n_dp)

    talk_mp = any(kind in ("split", "cast") for kind in kinds)
    talk_dp = "swap" in kinds
    talk_ring = "ring" in kinds
    barrier = pltpu.get_barrier_semaphore()
    greeted = 0
    if talk_mp:
        for offset in range(1, n_mp):
            pl.semaphore_signal(
                barrier, inc=1, device_id={"mp": (my_mp + offset) % n_mp}, device_id_type=MESH_ID
            )
            greeted += 1
    if talk_dp:
        for offset in range(1, n_dp):
            pl.semaphore_signal(
                barrier, inc=1, device_id={"dp": (my_dp + offset) % n_dp}, device_id_type=MESH_ID
            )
            greeted += 1
    elif talk_ring:
        for way in (1, n_dp - 1):
            pl.semaphore_signal(
                barrier,
                inc=1,
                device_id={"dp": ring_index((place + way) % n_dp, n_dp)},
                device_id_type=MESH_ID,
            )
            greeted += 1
    pl.semaphore_wait(barrier, greeted)

    def ring_copies(item, step):
        source, landing = ins[item], outs[item]
        parts = ring_parts(source.shape[0])
        made = {}
        for way, chunk in ring_step(parts, step, n_dp):
            origin = ring_index((place + (n_dp - step if way == 0 else step)) % n_dp, n_dp)
            target = ring_index((place + (1 if way == 0 else n_dp - 1)) % n_dp, n_dp)
            rows = pl.ds(*parts[chunk])
            spot = landing.at[origin, rows]
            made[way, chunk] = pltpu.make_async_remote_copy(
                src_ref=source.at[rows] if step == 0 else spot,
                dst_ref=spot,
                send_sem=sems[2 * item].at[step, chunk, way],
                recv_sem=sems[2 * item + 1].at[step, chunk, way],
                device_id={"dp": target},
                device_id_type=MESH_ID,
            )
        return made

    rings = [item for item in range(count) if kinds[item] == "ring"]
    flights = {item: ring_copies(item, 0) for item in rings}
    for item in rings:
        for copy in flights[item].values():
            copy.start()
    direct = []
    keeps = []
    for item, kind in enumerate(kinds):
        source, landing = ins[item], outs[item]
        if kind == "ring":
            keeps.append(pltpu.make_async_copy(source, landing.at[my_dp], local_sem.at[item]))
            continue
        size, mine, axis = (n_dp, my_dp, "dp") if kind == "swap" else (n_mp, my_mp, "mp")
        for offset in range(1, size):
            peer = (mine + offset) % size
            copy = pltpu.make_async_remote_copy(
                src_ref=source if kind == "cast" else source.at[peer],
                dst_ref=landing.at[mine],
                send_sem=sems[2 * item].at[offset],
                recv_sem=sems[2 * item + 1].at[offset],
                device_id={axis: peer},
                device_id_type=MESH_ID,
            )
            copy.start()
            direct.append(copy)
        keeps.append(
            pltpu.make_async_copy(
                source if kind == "cast" else source.at[mine], landing.at[mine], local_sem.at[item]
            )
        )
    for keep in keeps:
        keep.start()
    sent = [copy for item in rings for copy in flights[item].values()]
    landed = []
    for step in range(1, n_dp // 2):
        for item in rings:
            following = ring_copies(item, step)
            for key, after in following.items():
                flights[item].pop(key).wait_recv()
                after.start()
            landed += flights[item].values()
            flights[item] = following
            sent += following.values()
    for item in rings:
        landed += flights[item].values()
    for copy in landed:
        copy.wait_recv()
    for copy in direct:
        copy.wait_recv()
    for copy in sent + direct:
        copy.wait_send()
    for keep in keeps:
        keep.wait()


def exchange(ident, *pairs):
    n_dp, n_mp = lax.axis_size("dp"), lax.axis_size("mp")
    kinds = tuple(kind for kind, _ in pairs)
    arrays = [array for _, array in pairs]
    shapes, scratch = [], []
    for kind, array in pairs:
        lead = {"ring": (n_dp,), "cast": (n_mp,), "split": (), "swap": ()}[kind]
        shapes.append(jax.ShapeDtypeStruct(lead + array.shape, array.dtype))
        if kind == "ring":
            slots = (n_dp // 2, len(ring_parts(array.shape[0])), 2)
        else:
            slots = (n_dp if kind == "swap" else n_mp,)
        scratch += [pltpu.SemaphoreType.DMA(slots), pltpu.SemaphoreType.DMA(slots)]
    scratch.append(pltpu.SemaphoreType.DMA((len(pairs),)))
    return pl.pallas_call(
        functools.partial(exchange_kernel, n_dp, n_mp, kinds),
        out_shape=shapes,
        in_specs=[pl.BlockSpec(memory_space=pltpu.VMEM)] * len(pairs),
        out_specs=[pl.BlockSpec(memory_space=pltpu.VMEM)] * len(pairs),
        scratch_shapes=scratch,
        compiler_params=pltpu.CompilerParams(collective_id=ident, has_side_effects=True),
        name="exchange%d" % ident,
    )(*arrays)


def attend(queries, key_rows, value_rows, allowed):
    scores = jnp.einsum(
        "sqhd,skhd->shqk", queries, key_rows, preferred_element_type=jnp.float32
    ) * HDIM ** (-0.5)
    weights = jnp.where(allowed[:, None, :, :], jnp.exp(scores), 0.0)
    shares = (weights / jnp.sum(weights, axis=-1, keepdims=True)).astype(jnp.bfloat16)
    context = jnp.einsum("shqk,skhd->sqhd", shares, value_rows, preferred_element_type=jnp.float32)
    return context.astype(jnp.bfloat16)


def dot32(left, right):
    return jnp.dot(left, right, preferred_element_type=jnp.float32)


def dot_turned(left, right):
    return lax.dot_general(
        left, right, (((1,), (1,)), ((), ())), preferred_element_type=jnp.float32
    )


def added(blocks):
    return jnp.sum(blocks.astype(jnp.float32), axis=0)


def tail(first, target, weight_mask, inner_weight, outer_weight, final_weight):
    highest = lax.Precision.HIGHEST
    active = jax.nn.silu(first).astype(jnp.bfloat16)
    inner = jnp.dot(active, inner_weight, preferred_element_type=jnp.float32, precision=highest)
    second = jax.nn.silu(inner).astype(jnp.bfloat16)
    hidden = first + jnp.dot(
        second, outer_weight, preferred_element_type=jnp.float32, precision=highest
    )
    third = jax.nn.silu(hidden).astype(jnp.bfloat16)
    predicted = jnp.dot(third, final_weight, preferred_element_type=jnp.float32, precision=highest)
    differ = predicted - target
    return 0.5 * jnp.sum(weight_mask * differ * differ)


def head_grads(first, inner_weight, outer_weight, final_weight, target, weight_mask):

    def head_loss(first_in, inner_in, outer_in, final_in):
        return tail(first_in, target, weight_mask, inner_in, outer_in, final_in)

    loss_value, pullback = jax.vjp(head_loss, first, inner_weight, outer_weight, final_weight)
    return pullback(jnp.ones((), jnp.float32))


def on_device(
    tokens,
    obs_mask,
    norm_gains,
    attn_in,
    attn_out,
    mlp_in,
    mlp_out,
    embodiment,
    levels,
    actions,
    noise,
    action_dims,
    head_read,
    head_act,
    time_table,
    block_in,
    block_out,
    head_out,
):
    model = tokens.shape[1]
    act = actions.shape[2]
    width = attn_in.shape[3]
    heads_local = width // HDIM
    samples_local, length = obs_mask.shape
    layer_count = attn_in.shape[0]
    n_mp, n_dp = lax.axis_size("mp"), lax.axis_size("dp")
    my_model, my_owner = lax.axis_index("mp"), lax.axis_index("dp")
    samples_group = samples_local * n_mp
    ident = iter(range(100))

    joined = [
        jnp.concatenate(
            [attn_in[layer, 0], attn_in[layer, 1], attn_in[layer, 2], attn_out[layer].T], axis=1
        )
        for layer in range(layer_count)
    ]
    lowered = [mlp_out[layer].T for layer in range(layer_count)]

    heads_dev = head_read.shape[0]
    slot_count = heads_dev * n_dp
    owners = embodiment[:, 0]
    table = plan()
    onto = (jnp.arange(slot_count)[:, None] == owners[None, :]).astype(jnp.bfloat16)
    spread_rows = jnp.einsum("es,rq->ersq", onto, jnp.eye(READ, dtype=jnp.bfloat16)).reshape(
        slot_count * READ, samples_group * READ
    )
    small = jnp.concatenate(
        [
            noisy_pair(levels, actions, noise, table),
            noise,
            (levels + 1)[..., None].astype(jnp.bfloat16),
        ],
        axis=-1,
    ).reshape(samples_group * READ, 2 * act + 1)
    small = jnp.pad(small, ((0, 0), (0, -small.shape[1] % 128)))
    small = dot32(spread_rows, small).astype(jnp.bfloat16)
    small = small.reshape(n_dp, heads_dev * READ, small.shape[1])

    residual = tokens.astype(jnp.float32)
    wide = None
    allowed = None
    mask_group = None
    got_small = None
    position = jnp.arange(length)
    for layer in range(layer_count):
        final = layer == layer_count - 1
        normed = normalize(residual, norm_gains[2 * layer]).astype(jnp.bfloat16)
        if layer == 0:
            sends = [("cast", normed), ("cast", obs_mask), ("swap", small), ("ring", joined[0])]
        else:
            sends = [("cast", normed)]
        if final:
            ends = residual.reshape(samples_local, length, model)[:, length - READ :, :]
            sends += [("cast", ends), ("ring", mlp_in[layer]), ("ring", lowered[layer])]
        got = list(exchange(next(ident), *sends))
        gathered = got.pop(0).reshape(-1, model)
        if layer == 0:
            mask_group = got.pop(0).reshape(samples_group, length)
            got_small = got.pop(0)
            wide = got.pop(0).reshape(model, -1)
            visible = (mask_group == 1) & (position < length - READ)[None, :]
            itself = position[:, None] == position[None, :]
            allowed = visible[:, None, :] | itself[None, :, :]
        if final:
            ends = got.pop(0).reshape(samples_group * READ, model)
            upper = got.pop(0).reshape(model, -1)
            lower = got.pop(0).reshape(model, -1)
            asking = gathered.reshape(samples_group, length, model)[:, length - READ :, :]
            queries = dot32(asking.reshape(-1, model), wide[:, :width]).astype(jnp.bfloat16)
            queries = queries.reshape(samples_group, READ, heads_local, HDIM)
            both = dot32(gathered, wide[:, width : 3 * width]).astype(jnp.bfloat16)
            keys_at = both[:, :width].reshape(samples_group, length, heads_local, HDIM)
            values_at = both[:, width:].reshape(samples_group, length, heads_local, HDIM)
            context = attend(queries, keys_at, values_at, allowed[:, length - READ :, :])
            partial_value = dot_turned(context.reshape(-1, width), wide[:, 3 * width :])
            (terms,) = exchange(next(ident), ("cast", partial_value.astype(jnp.bfloat16)))
            ends = ends + added(terms)
            normed = normalize(ends, norm_gains[2 * layer + 1]).astype(jnp.bfloat16)
            hidden = jax.nn.gelu(dot32(normed, upper), approximate=True).astype(jnp.bfloat16)
            partial_value = dot_turned(hidden, lower)
            (terms,) = exchange(next(ident), ("cast", partial_value.astype(jnp.bfloat16)))
            ends = ends + added(terms)
            break
        projected = dot32(gathered, wide[:, : 3 * width]).astype(jnp.bfloat16)
        split = [
            projected[:, part * width : (part + 1) * width].reshape(
                samples_group, length, heads_local, HDIM
            )
            for part in range(3)
        ]
        context = attend(split[0], split[1], split[2], allowed).reshape(-1, width)
        partial_value = dot_turned(context, wide[:, 3 * width :]).astype(jnp.bfloat16)
        terms, upper = exchange(
            next(ident),
            ("split", partial_value.reshape(n_mp, -1, model)),
            ("ring", mlp_in[layer]),
        )
        residual = residual + added(terms)
        normed = normalize(residual, norm_gains[2 * layer + 1]).astype(jnp.bfloat16)
        gathered, lower = exchange(next(ident), ("cast", normed), ("ring", lowered[layer]))
        raised = dot32(gathered.reshape(-1, model), upper.reshape(model, -1))
        hidden = jax.nn.gelu(raised, approximate=True).astype(jnp.bfloat16)
        partial_value = dot_turned(hidden, lower.reshape(model, -1)).astype(jnp.bfloat16)
        terms, wide = exchange(
            next(ident),
            ("split", partial_value.reshape(n_mp, -1, model)),
            ("ring", joined[layer + 1]),
        )
        wide = wide.reshape(model, -1)
        residual = residual + added(terms)

    readouts = normalize(ends, norm_gains[2 * layer_count]).astype(jnp.bfloat16)
    send = dot32(spread_rows, readouts).astype(jnp.bfloat16)
    (got_features,) = exchange(
        next(ident), ("swap", send.reshape(n_dp, heads_dev * READ, model))
    )

    def by_head(values):
        values = values.reshape(n_dp, heads_dev, READ, values.shape[-1])
        return jnp.moveaxis(values, 1, 0).reshape(heads_dev, n_dp * READ, values.shape[-1])

    head_features = by_head(got_features)
    head_small = by_head(got_small)
    head_noisy = head_small[..., :act]
    head_target = head_small[..., act : 2 * act].astype(jnp.float32)
    head_levels = head_small[..., 2 * act].astype(jnp.int32) - 1
    head_onehot = (head_levels[..., None] == jnp.arange(LEVELS)).astype(jnp.bfloat16)
    slot_ids = my_owner * heads_dev + jnp.arange(heads_dev)
    dims_here = jnp.sum(
        jnp.where(jnp.arange(EMB)[None, :] == slot_ids[:, None], action_dims[None, :], 0), axis=1
    )
    column = jnp.arange(act) % ADIM_MAX
    weight_mask = (head_levels >= 0).astype(jnp.float32)[..., None] * (
        column[None, None, :] < dims_here[:, None, None]
    ).astype(jnp.float32)
    others = jnp.einsum("hna,hac->hnc", head_noisy, head_act, preferred_element_type=jnp.float32)
    others = others + jnp.einsum(
        "hnl,hlc->hnc", head_onehot, time_table, preferred_element_type=jnp.float32
    )
    first = (
        jnp.einsum("hnd,hdc->hnc", head_features, head_read, preferred_element_type=jnp.float32)
        + others
    )
    grad_first, grad_inner, grad_outer, grad_final = jax.vmap(head_grads)(
        first,
        block_in.astype(jnp.float32),
        block_out.astype(jnp.float32),
        head_out.astype(jnp.float32),
        head_target,
        weight_mask,
    )
    grad_bf = grad_first.astype(jnp.bfloat16)
    backward = jnp.einsum(
        "hnc,hdc->hnd", grad_bf, head_read, preferred_element_type=jnp.float32
    ).astype(jnp.bfloat16)
    backward = jnp.moveaxis(backward.reshape(heads_dev, n_dp, READ, model), 0, 1)
    (arrived,) = exchange(
        next(ident), ("swap", backward.reshape(n_dp, heads_dev * READ, model))
    )
    mine = lax.dynamic_slice_in_dim(
        spread_rows, my_model * (samples_local * READ), samples_local * READ, 1
    )
    returned = lax.dot_general(
        mine,
        arrived.reshape(slot_count * READ, model),
        (((0,), (0,)), ((), ())),
        preferred_element_type=jnp.float32,
    ).astype(jnp.bfloat16)
    feature_width = model // n_mp
    own_features = lax.dynamic_slice_in_dim(
        head_features, my_model * feature_width, feature_width, 2
    )
    grad_readin = jnp.einsum(
        "hnd,hnc->hdc", own_features, grad_bf, preferred_element_type=jnp.float32
    )
    grad_actin = jnp.einsum("hna,hnc->hac", head_noisy, grad_bf, preferred_element_type=jnp.float32)
    grad_timein = jnp.einsum(
        "hnl,hnc->hlc", head_onehot, grad_bf, preferred_element_type=jnp.float32
    )
    return (
        returned.reshape(samples_local, READ, model),
        grad_readin,
        grad_actin,
        grad_timein,
        grad_inner,
        grad_outer,
        grad_final,
    )


def solution(mesh):
    placed = (
        P(("dp", "mp"), None),
        P(("dp", "mp"), None),
        P(),
        P(None, None, "dp", "mp"),
        P(None, "mp", "dp"),
        P(None, "dp", "mp"),
        P(None, "mp", "dp"),
        P("dp", None),
        P("dp", None),
        P("dp", None, None),
        P("dp", None, None),
        P(),
        P("dp", None, None),
        P("dp", None, None),
        P("dp", None, None),
        P("dp", None, None),
        P("dp", None, None),
        P("dp", None, None),
    )
    return jax.shard_map(
        on_device,
        mesh=mesh,
        in_specs=placed,
        out_specs=(
            P(("dp", "mp"), None, None),
            P("dp", "mp", None),
            P("dp", None, None),
            P("dp", None, None),
            P("dp", None, None),
            P("dp", None, None),
            P("dp", None, None),
        ),
        check_vma=False,
    )
```
